128 devices in a mesh: dp: 1, hp: 2 (over core), cp: 64 (over z, y, x).
Axes of the slice: x: 4, y: 4, z: 4, core: 2. Of those that a mesh axis runs over, the one named last changes fastest.
Arguments:
- latent: bfloat16 [1536, 12, 128, 128], P(('dp', 'cp'), 'hp')
- conv_w: bfloat16 [4, 3, 3, 3, 128, 128], replicated
- conv_b: float32 [4, 128], replicated
- gn_gamma: float32 [4, 128], replicated
- gn_beta: float32 [4, 128], replicated
Outputs:
- output: bfloat16 [1536, 12, 128, 128], P(('dp', 'cp'), 'hp')
All inputs are finite; a program needn't handle non-finite values.
Results may differ from the reference program's by a relative error of at most 0.0101423.
Values are sent between devices in bfloat16 or wider.
A program may use at most 1 GiB of HBM per device.

```python
import jax
import jax.numpy as jnp
from jax import lax

FRAMES = 1536
HEIGHT = 12
LAT_WIDTH = 128
CHANNELS = 128
GROUPS = 32
EPS = 1e-6


def setup_inputs(seed: int = 0, part: int = 0) -> dict:
    root_key = jax.random.key(seed)
    part_key = jax.random.fold_in(root_key, part)
    key_noise, key_fscale, key_fshift, key_rscale = jax.random.split(part_key, 4)
    key_kernel, key_bias, key_gamma, key_beta = jax.random.split(jax.random.key(seed + 1), 4)
    base_noise = jax.random.normal(key_noise, (FRAMES, HEIGHT, LAT_WIDTH, CHANNELS), jnp.float32)
    frame_scale = jnp.exp(0.5 * jax.random.normal(key_fscale, (FRAMES, 1, 1, 1), jnp.float32))
    frame_shift = 0.7 * jax.random.normal(key_fshift, (FRAMES, 1, 1, CHANNELS), jnp.float32)
    row_scale = jnp.exp(0.4 * jax.random.normal(key_rscale, (1, HEIGHT, 1, 1), jnp.float32))
    latent = ((base_noise + frame_shift) * frame_scale * row_scale).astype(jnp.bfloat16)
    fan_in = 27 * CHANNELS
    conv_w = (jax.random.normal(key_kernel, (4, 3, 3, 3, CHANNELS, CHANNELS), jnp.float32) * fan_in ** -0.5).astype(jnp.bfloat16)
    conv_b = 0.5 * jax.random.normal(key_bias, (4, CHANNELS), jnp.float32)
    gn_gamma = 1.0 + 0.3 * jax.random.normal(key_gamma, (4, CHANNELS), jnp.float32)
    gn_beta = 0.3 * jax.random.normal(key_beta, (4, CHANNELS), jnp.float32)
    return {"latent": latent, "conv_w": conv_w, "conv_b": conv_b, "gn_gamma": gn_gamma, "gn_beta": gn_beta}


def norm_silu(video, gamma, beta):
    per_group = CHANNELS // GROUPS
    grouped = video.reshape(FRAMES, HEIGHT, LAT_WIDTH, GROUPS, per_group).astype(jnp.float32)
    norm_count = FRAMES * HEIGHT * LAT_WIDTH * per_group
    mean_val = jnp.sum(grouped, axis=(0, 1, 2, 4)) / norm_count
    variance = jnp.sum(grouped * grouped, axis=(0, 1, 2, 4)) / norm_count - mean_val * mean_val
    inv_std = lax.rsqrt(variance + EPS)
    gamma_g = gamma.reshape(GROUPS, per_group)
    scale_c = (inv_std[:, None] * gamma_g).reshape(CHANNELS)
    shift_c = (beta.reshape(GROUPS, per_group) - (mean_val * inv_std)[:, None] * gamma_g).reshape(CHANNELS)
    return jax.nn.silu(video.astype(jnp.float32) * scale_c + shift_c).astype(jnp.bfloat16)


def causal_conv(video, kernel, bias_vec):
    padded = jnp.concatenate([video[:1], video[:1], video], axis=0)
    kernel_f = kernel.astype(jnp.float32)

    def one_frame(frame_idx):
        window = lax.dynamic_slice_in_dim(padded, frame_idx, 3, axis=0).astype(jnp.float32)
        conv_out = lax.conv_general_dilated(window[None], kernel_f, (1, 1, 1), ((0, 0), (1, 1), (1, 1)), dimension_numbers=("NDHWC", "DHWIO", "NDHWC"))
        return (conv_out[0, 0] + bias_vec).astype(jnp.bfloat16)

    return lax.map(one_frame, jnp.arange(FRAMES))


def reference(latent, conv_w, conv_b, gn_gamma, gn_beta):
    residual = latent
    for block_idx in range(2):
        hidden = residual
        for sub_idx in range(2):
            layer_idx = 2 * block_idx + sub_idx
            activated = norm_silu(hidden, gn_gamma[layer_idx], gn_beta[layer_idx])
            hidden = causal_conv(activated, conv_w[layer_idx], conv_b[layer_idx])
        residual = (residual.astype(jnp.float32) + hidden.astype(jnp.float32)).astype(jnp.bfloat16)
    return residual
```

```python
import functools

import jax
import jax.numpy as jnp
from jax import lax
from jax.experimental import pallas as pl
from jax.experimental.pallas import tpu as pltpu
from jax.sharding import PartitionSpec as P

MESH = pl.DeviceIdType.MESH
GROUPS = 32
EPS = 1e-6
FRAMES = 24
ROWS = 6
W = 128
C = 128
TRIPS = 4
CHUNKS = ((22, 4), (16, 6), (10, 6), (4, 6), (2, 2))
SIDE = 64
BF = jnp.bfloat16
F32 = jnp.float32


def kernel(count, n_cp, lat, w_hbm, bias, gamma, beta, out, buf_a, buf_b, act0, act1, act2, wts, tmp, stat_out, stat_in,
           x_sem, w_sem, out_sem, row_send, row_recv, frame_send, frame_recv, stat_send, stat_recv):
    me = lax.axis_index("cp")
    hp = lax.axis_index("hp")
    acts = (act0, act1, act2)
    cx, cy, cz = me % 4, (me // 4) % 4, me // 16
    partner = {"hp": 1 - hp}
    after = {"cp": (me + 1) % n_cp}
    before = {"cp": (me + n_cp - 1) % n_cp}

    def at(x, y, z):
        return (z * 4 + y) * 4 + x

    ring = (2, 1, 3)
    x_peers = [((cx + d) % 4, h) for d in ring for h in (0, 1)]
    y_peers = [(cy + d) % 4 for d in ring]
    z_peers = [(cz + d) % 4 for d in ring]

    def x_load(c):
        f, n = CHUNKS[c]
        return pltpu.make_async_copy(lat.at[pl.ds(f - 2, n)], buf_a.at[pl.ds(f, n), pl.ds(0, ROWS)], x_sem.at[c])

    def w_load(l):
        return pltpu.make_async_copy(w_hbm.at[l], wts.at[l], w_sem.at[l])

    for c in range(5):
        x_load(c).start()
    for l in range(4):
        w_load(l).start()

    barrier = pltpu.get_barrier_semaphore()
    greet = [partner, after, before]
    greet += [{"cp": at(x, cy, cz), "hp": h} for x, h in x_peers]
    greet += [{"cp": at(cx, y, cz)} for y in y_peers]
    greet += [{"cp": at(cx, cy, z)} for z in z_peers]
    for d in greet:
        pl.semaphore_signal(barrier, inc=1, device_id=d, device_id_type=MESH)

    def row_copy(s, c):
        buf = (buf_a, buf_b)[s % 2]
        f, n = CHUNKS[c]
        edge = (ROWS - 1) * (1 - hp)
        return pltpu.make_async_remote_copy(
            src_ref=buf.at[pl.ds(f, n), pl.ds(edge, 1)], dst_ref=buf.at[pl.ds(f, n), pl.ds(ROWS, 1)],
            send_sem=row_send.at[s, c], recv_sem=row_recv.at[s, c], device_id=partner, device_id_type=MESH)

    def frame_copy(s):
        buf = (buf_a, buf_b)[s % 2]
        return pltpu.make_async_remote_copy(
            src_ref=buf.at[pl.ds(24, 2)], dst_ref=buf.at[pl.ds(0, 2)],
            send_sem=frame_send.at[s], recv_sem=frame_recv.at[s], device_id=after, device_id_type=MESH)

    def out_copy(c):
        f, n = CHUNKS[c]
        return pltpu.make_async_copy(buf_a.at[pl.ds(f, n), pl.ds(0, ROWS)], out.at[pl.ds(f - 2, n)], out_sem.at[c])

    def stat_copy(s, k, src, slot, device):
        return pltpu.make_async_remote_copy(
            src_ref=stat_out.at[s, src], dst_ref=stat_in.at[s, slot],
            send_sem=stat_send.at[s, k], recv_sem=stat_recv.at[s, slot], device_id=device, device_id_type=MESH)

    row_id = lax.broadcasted_iota(jnp.int32, (8, C), 0)
    lane_id = lax.broadcasted_iota(jnp.int32, (8, C), 1)

    def reduce_stats(s, s1, s2, mid):
        v1 = jnp.sum(s1, axis=0, keepdims=True)
        v2 = jnp.sum(s2, axis=0, keepdims=True)
        part = jnp.where(row_id == 0, v1, jnp.where(row_id == 1, v2, 0.0))
        phases = (
            (cx * 2 + hp, 0, 8, [(x * 2 + h, {"cp": at(x, cy, cz), "hp": h}) for x, h in x_peers] + [(cx * 2 + 1 - hp, partner)]),
            (cy, 8, 4, [(y, {"cp": at(cx, y, cz)}) for y in y_peers]),
            (cz, 12, 4, [(z, {"cp": at(cx, cy, z)}) for z in z_peers]),
        )
        k = 0
        sends = []
        for ph, (own, base, n, peers) in enumerate(phases):
            stat_out[s, ph] = part
            stat_in[s, base + own] = part
            first = k
            for _, device in peers:
                c = stat_copy(s, k, ph, base + own, device)
                c.start()
                sends.append(c)
                k += 1
            if ph == 0:
                mid()
            for i, (slot, device) in enumerate(peers):
                stat_copy(s, first + i, ph, base + slot, device).wait_recv()
            part = stat_in[s, base]
            for i in range(1, n):
                part = part + stat_in[s, base + i]
        for c in sends:
            c.wait_send()
        return part

    def coefficients(l, part):
        pair = part + jnp.where(lane_id % 2 == 0, pltpu.roll(part, C - 1, 1), pltpu.roll(part, 1, 1))
        group = pair + jnp.where(lane_id % 4 < 2, pltpu.roll(pair, C - 2, 1), pltpu.roll(pair, 2, 1))
        mean = group[0:1] / count
        var = group[1:2] / count - mean * mean
        inv = lax.rsqrt(var + EPS)
        g = gamma[l:l + 1]
        scale = inv * g
        shift = beta[l:l + 1] - mean * inv * g
        return jnp.broadcast_to(0.5 * scale, (8, C)), jnp.broadcast_to(0.5 * shift, (8, C))

    col8 = lax.broadcasted_iota(jnp.int32, (W, C), 0)
    halo_row = 7 * (1 - hp)

    def norm_row(src, dst, q, e, r, coef):
        scale, shift = coef
        f = jnp.maximum(24 - 2 * q, 0) + e
        f = jnp.where((q >= 12) & (me == 0), 2, f)
        v = src[f, r].astype(F32).reshape(W // 8, 8, C)
        u = (v * scale[None] + shift[None]).reshape(W, C)
        a = u + u * jnp.tanh(u)
        row = halo_row if r == ROWS else r + 1
        dst[1, e, row] = a.astype(BF)
        dst[0, e, row] = jnp.where(col8 == 0, 0.0, pltpu.roll(a, 1, 0)).astype(BF)
        dst[2, e, row] = jnp.where(col8 == W - 1, 0.0, pltpu.roll(a, W - 1, 0)).astype(BF)

    def tile(l, n, m):
        def w(k, di, dj):
            return wts[l, k * 9 + di * 3 + dj]

        def block(a, b, c, d):
            return jnp.concatenate([jnp.concatenate([a, b], 1), jnp.concatenate([c, d], 1)], 0)

        if n < 9:
            di, dj = n // 3, n % 3
            return block(w(1, di, dj), w(0, di, dj), w(2, di, dj), w(1, di, dj))
        dj, half = (n - 9) % 3, (n - 9) // 3
        k = 0 if m == 0 else 2
        if half == 0:
            return block(w(k, 1, dj), w(k, 0, dj), w(k, 2, dj), w(k, 1, dj))
        zero = jnp.zeros((C, C), BF)
        return block(w(k, 0, dj), zero, zero, w(k, 2, dj))

    def lhs(cur, prv, n, m, j):
        if n < 9:
            di, dj = n // 3, n % 3
            i = 3 * m + j + di
            return jnp.concatenate([prv[dj, 1, i], cur[dj, 0, i]], 1)
        dj, half = (n - 9) % 3, (n - 9) // 3
        frame = prv.at[dj, 0] if m == 0 else cur.at[dj, 1]
        i = 2 * j
        if half == 0:
            return jnp.concatenate([frame[i + 1], frame[i + 2]], 1)
        return jnp.concatenate([frame[i], frame[i + 3]], 1)

    def sum8(v):
        return jnp.sum(v.reshape(W // 8, 8, C), axis=0)

    def layer(l, coef):
        src = (buf_a, buf_b)[l % 2]
        dst = (buf_a, buf_b)[1 - l % 2]
        residual = l % 2 == 1
        last = l == 3
        bias2 = jnp.concatenate([bias[l:l + 1], bias[l:l + 1]], 1)

        def finish(q, e, j, full, v, sums):
            f = 24 - 2 * q + e
            s1, s2 = sums
            for half in range(2):
                o = 2 * j + half
                h = (full[o * W:(o + 1) * W, e * C:(e + 1) * C] + v[j * W:(j + 1) * W, half * C:(half + 1) * C]).astype(BF)
                if residual:
                    h = (dst[f, o].astype(F32) + h.astype(F32)).astype(BF)
                dst[f, o] = h
                if not last:
                    hf = h.astype(F32)
                    s1 = s1 + sum8(hf)
                    s2 = s2 + sum8(hf * hf)
            return s1, s2

        def trip(it, sums):
            def wait_rows(c):
                row_copy(l, c).wait_recv()

            for i in range(3):
                @pl.when(it == i)
                def _(i=i):
                    wait_rows(i + 1)

            @pl.when(it == 3)
            def _():
                wait_rows(4)
                frame_copy(l).wait_recv()

            for i in range(1, 4):
                @pl.when(it == i)
                def _(i=i):
                    if last:
                        out_copy(i - 1).start()
                    else:
                        row_copy(l + 1, i - 1).start()
                        if i == 2:
                            row_copy(l + 1, 0).wait_recv()
                            frame_copy(l + 1).start()

            for k in range(3):
                q = 3 * it + k
                cur, prv, nxt = acts[k], acts[(k + 1) % 3], acts[(k + 2) % 3]
                full = jnp.dot(
                    jnp.concatenate([jnp.concatenate([lhs(cur, prv, n, m, j) for n in range(9)], 1) for m in range(2) for j in range(3)], 0),
                    jnp.concatenate([tile(l, n, 0) for n in range(9)], 0), preferred_element_type=F32) + bias2
                half = [jnp.dot(
                    jnp.concatenate([jnp.concatenate([lhs(cur, prv, n, m, j) for n in range(9, 15)], 1) for j in range(3)], 0),
                    jnp.concatenate([tile(l, n, m) for n in range(9, 15)], 0), preferred_element_type=F32) for m in range(2)]
                for e in range(2):
                    for r in range(7):
                        norm_row(src, nxt, q + 2, e, r, coef)
                for e in range(2):
                    for j in range(3):
                        sums = finish(q, e, j, full, half[e], sums)
            return sums

        for q in range(2):
            for e in range(2):
                for r in range(7):
                    norm_row(src, acts[q], q, e, r, coef)
        zero = jnp.zeros((8, C), F32)
        sums = lax.fori_loop(0, TRIPS, trip, (zero, zero))
        if last:
            out_copy(3).start()
        else:
            row_copy(l + 1, 3).start()
        for c in range(5):
            row_copy(l, c).wait_send()
        frame_copy(l).wait_send()
        if last:
            out_copy(4).start()
        return sums

    def body():
        blank = jnp.zeros((W, C), BF)
        for act in acts:
            for dj in range(3):
                for e in range(2):
                    for r in (0, 7):
                        act[dj, e, r] = blank

        sums = (jnp.zeros((8, C), F32), jnp.zeros((8, C), F32))
        for c, (f, n) in enumerate(CHUNKS):
            x_load(c).wait()

            def add(i, sums, f=f):
                s1, s2 = sums
                for r in range(ROWS):
                    v = buf_a[f + i, r].astype(F32)
                    s1 = s1 + sum8(v)
                    s2 = s2 + sum8(v * v)
                return s1, s2

            sums = lax.fori_loop(0, n, add, sums)

        pl.semaphore_wait(barrier, len(greet))
        for l in range(4):
            w_load(l).wait()
        for l in range(4):
            def mid(l=l):
                if l == 0:
                    for c in range(5):
                        row_copy(0, c).start()
                    row_copy(0, 0).wait_recv()
                    frame_copy(0).start()
                else:
                    row_copy(l, 4).start()

            part = reduce_stats(l, *sums, mid)
            sums = layer(l, coefficients(l, part))
        for c in range(5):
            out_copy(c).wait()

    body()


def solution(mesh):
    n_cp, n_hp = mesh.shape["cp"], mesh.shape["hp"]

    def local(lat, conv_w, conv_b, gn_gamma, gn_beta):
        count = float(FRAMES * n_cp * ROWS * n_hp * W * (C // GROUPS))
        any_spec = pl.BlockSpec(memory_space=pl.ANY)
        vmem = pl.BlockSpec(memory_space=pltpu.VMEM)
        dma = pltpu.SemaphoreType.DMA
        return pl.pallas_call(
            functools.partial(kernel, count, n_cp),
            out_shape=jax.ShapeDtypeStruct((FRAMES, ROWS, W, C), BF),
            in_specs=[any_spec, any_spec, vmem, vmem, vmem],
            out_specs=any_spec,
            scratch_shapes=[
                pltpu.VMEM((FRAMES + 4, ROWS + 1, W, C), BF),
                pltpu.VMEM((FRAMES + 4, ROWS + 1, W, C), BF),
                pltpu.VMEM((3, 2, ROWS + 2, W, C), BF),
                pltpu.VMEM((3, 2, ROWS + 2, W, C), BF),
                pltpu.VMEM((3, 2, ROWS + 2, W, C), BF),
                pltpu.VMEM((4, 27, C, C), BF),
                pltpu.VMEM((ROWS, W, 2 * C), F32),
                pltpu.VMEM((4, 3, 8, C), F32),
                pltpu.VMEM((4, 16, 8, C), F32),
                dma((5,)), dma((4,)), dma((5,)),
                dma((4, 5)), dma((4, 5)), dma((4,)), dma((4,)),
                dma((4, 13)), dma((4, 16)),
            ],
            compiler_params=pltpu.CompilerParams(collective_id=0, has_side_effects=True, vmem_limit_bytes=60 * 2**20),
        )(lat, conv_w.reshape(4, 27, C, C), conv_b, gn_gamma, gn_beta)

    video = P(("dp", "cp"), "hp", None, None)
    return jax.shard_map(local, mesh=mesh, in_specs=(video, P(), P(), P(), P()), out_specs=video, check_vma=False)
```

```python
import functools

import jax
import jax.numpy as jnp
from jax import lax
from jax.experimental import pallas as pl
from jax.experimental.pallas import tpu as pltpu
from jax.sharding import PartitionSpec as P

MESH = pl.DeviceIdType.MESH
GROUPS = 32
EPS = 1e-6
FRAMES = 24
ROWS = 6
W = 128
C = 128
TRIPS = 4
CHUNKS = ((22, 4), (16, 6), (10, 6), (4, 6), (2, 2))
SIDE = 64
BF = jnp.bfloat16
F32 = jnp.float32


def kernel(count, n_cp, lat, w_hbm, bias, gamma, beta, out, buf_a, buf_b, act0, act1, act2, wts, stat_out, stat_in,
           x_sem, w_sem, out_sem, row_send, row_recv, frame_send, frame_recv, stat_send, stat_recv):
    me = lax.axis_index("cp")
    hp = lax.axis_index("hp")
    acts = (act0, act1, act2)
    partner = {"hp": 1 - hp}
    after = {"cp": (me + 1) % n_cp}

    def peer(j):
        return (me + 1 + (j + n_cp // 2 - 1) % (n_cp - 1)) % n_cp

    def x_load(c):
        f, n = CHUNKS[c]
        return pltpu.make_async_copy(lat.at[pl.ds(f - 2, n)], buf_a.at[pl.ds(f, n), pl.ds(0, ROWS)], x_sem.at[c])

    def w_load(l):
        return pltpu.make_async_copy(w_hbm.at[l], wts.at[l], w_sem.at[l])

    for c in range(5):
        x_load(c).start()
    for l in range(4):
        w_load(l).start()

    barrier = pltpu.get_barrier_semaphore()
    def greet(j, _):
        pl.semaphore_signal(barrier, inc=1, device_id={"cp": peer(j)}, device_id_type=MESH)
        return _

    pl.semaphore_signal(barrier, inc=1, device_id=partner, device_id_type=MESH)
    lax.fori_loop(0, n_cp - 1, greet, 0)

    def row_copy(s, c):
        buf = (buf_a, buf_b)[s % 2]
        f, n = CHUNKS[c]
        edge = (ROWS - 1) * (1 - hp)
        return pltpu.make_async_remote_copy(
            src_ref=buf.at[pl.ds(f, n), pl.ds(edge, 1)], dst_ref=buf.at[pl.ds(f, n), pl.ds(ROWS, 1)],
            send_sem=row_send.at[s, c], recv_sem=row_recv.at[s, c], device_id=partner, device_id_type=MESH)

    def frame_copy(s):
        buf = (buf_a, buf_b)[s % 2]
        return pltpu.make_async_remote_copy(
            src_ref=buf.at[pl.ds(24, 2)], dst_ref=buf.at[pl.ds(0, 2)],
            send_sem=frame_send.at[s], recv_sem=frame_recv.at[s], device_id=after, device_id_type=MESH)

    def out_copy(c):
        f, n = CHUNKS[c]
        return pltpu.make_async_copy(buf_a.at[pl.ds(f, n), pl.ds(0, ROWS)], out.at[pl.ds(f - 2, n)], out_sem.at[c])

    def chip_copy(s, j, slot):
        p = peer(j)
        return pltpu.make_async_remote_copy(
            src_ref=stat_out.at[s % 2, 0], dst_ref=stat_in.at[s % 2, p if slot is None else slot],
            send_sem=stat_send.at[s % 2, p], recv_sem=stat_recv.at[s % 2, p if slot is None else slot],
            device_id={"cp": p}, device_id_type=MESH)

    def core_copy(s):
        return pltpu.make_async_remote_copy(
            src_ref=stat_out.at[s % 2, 1], dst_ref=stat_in.at[s % 2, n_cp], send_sem=stat_send.at[s % 2, n_cp],
            recv_sem=stat_recv.at[s % 2, n_cp], device_id=partner, device_id_type=MESH)

    row_id = lax.broadcasted_iota(jnp.int32, (8, C), 0)
    lane_id = lax.broadcasted_iota(jnp.int32, (8, C), 1)

    def reduce_stats(s, s1, s2, mid):
        part = jnp.concatenate([jnp.sum(s1, axis=0, keepdims=True), jnp.sum(s2, axis=0, keepdims=True)], 0)
        stat_out[s % 2, 0] = part
        stat_in[s % 2, me] = part

        def send(j, _):
            chip_copy(s, j, me).start()
            return _

        def wait(j, _):
            chip_copy(s, j, None).wait()
            return _

        lax.fori_loop(0, n_cp - 1, send, 0)
        mid()
        lax.fori_loop(0, n_cp - 1, wait, 0)
        terms = [stat_in[s % 2, i] for i in range(n_cp)]
        while len(terms) > 1:
            terms = [a + b for a, b in zip(terms[::2], terms[1::2])]
        stat_out[s % 2, 1] = terms[0]
        core_copy(s).start()
        core_copy(s).wait()
        return terms[0] + stat_in[s % 2, n_cp]

    def coefficients(l, part):
        part = jnp.where(row_id == 0, part[0:1], part[1:2])
        pair = part + jnp.where(lane_id % 2 == 0, pltpu.roll(part, C - 1, 1), pltpu.roll(part, 1, 1))
        group = pair + jnp.where(lane_id % 4 < 2, pltpu.roll(pair, C - 2, 1), pltpu.roll(pair, 2, 1))
        mean = group[0:1] / count
        var = group[1:2] / count - mean * mean
        inv = lax.rsqrt(var + EPS)
        g = gamma[l:l + 1]
        scale = inv * g
        shift = beta[l:l + 1] - mean * inv * g
        return jnp.broadcast_to(0.5 * scale, (8, C)), jnp.broadcast_to(0.5 * shift, (8, C))

    col8 = lax.broadcasted_iota(jnp.int32, (W, C), 0)
    halo_row = 7 * (1 - hp)

    def norm_row(src, dst, q, e, r, coef):
        scale, shift = coef
        f = jnp.maximum(24 - 2 * q, 0) + e
        f = jnp.where((q >= 12) & (me == 0), 2, f)
        v = src[f, r].astype(F32).reshape(W // 8, 8, C)
        u = (v * scale[None] + shift[None]).reshape(W, C)
        a = u + u * jnp.tanh(u)
        row = halo_row if r == ROWS else r + 1
        dst[1, e, row] = a.astype(BF)
        dst[0, e, row] = jnp.where(col8 == 0, 0.0, pltpu.roll(a, 1, 0)).astype(BF)
        dst[2, e, row] = jnp.where(col8 == W - 1, 0.0, pltpu.roll(a, W - 1, 0)).astype(BF)

    def tile(l, n, m):
        def w(k, di, dj):
            return wts[l, k * 9 + di * 3 + dj]

        def block(a, b, c, d):
            return jnp.concatenate([jnp.concatenate([a, b], 1), jnp.concatenate([c, d], 1)], 0)

        if n < 9:
            di, dj = n // 3, n % 3
            return block(w(1, di, dj), w(0, di, dj), w(2, di, dj), w(1, di, dj))
        dj, half = (n - 9) % 3, (n - 9) // 3
        k = 0 if m == 0 else 2
        if half == 0:
            return block(w(k, 1, dj), w(k, 0, dj), w(k, 2, dj), w(k, 1, dj))
        zero = jnp.zeros((C, C), BF)
        return block(w(k, 0, dj), zero, zero, w(k, 2, dj))

    def lhs(cur, prv, n, m, j):
        if n < 9:
            di, dj = n // 3, n % 3
            i = 3 * m + j + di
            return jnp.concatenate([prv[dj, 1, i], cur[dj, 0, i]], 1)
        dj, half = (n - 9) % 3, (n - 9) // 3
        frame = prv.at[dj, 0] if m == 0 else cur.at[dj, 1]
        i = 2 * j
        if half == 0:
            return jnp.concatenate([frame[i + 1], frame[i + 2]], 1)
        return jnp.concatenate([frame[i], frame[i + 3]], 1)

    def sum8(v):
        return jnp.sum(v.reshape(W // 8, 8, C), axis=0)

    def layer(l, coef):
        src = (buf_a, buf_b)[l % 2]
        dst = (buf_a, buf_b)[1 - l % 2]
        residual = l % 2 == 1
        last = l == 3
        bias2 = jnp.concatenate([bias[l:l + 1], bias[l:l + 1]], 1)

        def finish(q, e, j, full, v, sums):
            f = 24 - 2 * q + e
            s1, s2 = sums
            for half in range(2):
                o = 2 * j + half
                h = (full[o * W:(o + 1) * W, e * C:(e + 1) * C] + v[j * W:(j + 1) * W, half * C:(half + 1) * C]).astype(BF)
                if residual:
                    h = (dst[f, o].astype(F32) + h.astype(F32)).astype(BF)
                dst[f, o] = h
                if not last:
                    hf = h.astype(F32)
                    s1 = s1 + sum8(hf)
                    s2 = s2 + sum8(hf * hf)
            return s1, s2

        def trip(it, sums):
            def wait_rows(c):
                row_copy(l, c).wait_recv()

            for i in range(3):
                @pl.when(it == i)
                def _(i=i):
                    wait_rows(i + 1)

            @pl.when(it == 3)
            def _():
                wait_rows(4)
                frame_copy(l).wait_recv()

            for i in range(1, 4):
                @pl.when(it == i)
                def _(i=i):
                    if last:
                        out_copy(i - 1).start()
                    else:
                        row_copy(l + 1, i - 1).start()
                        if i == 2:
                            row_copy(l + 1, 0).wait_recv()
                            frame_copy(l + 1).start()

            for k in range(3):
                q = 3 * it + k
                cur, prv, nxt = acts[k], acts[(k + 1) % 3], acts[(k + 2) % 3]
                full = jnp.dot(
                    jnp.concatenate([jnp.concatenate([lhs(cur, prv, n, m, j) for n in range(9)], 1) for m in range(2) for j in range(3)], 0),
                    jnp.concatenate([tile(l, n, 0) for n in range(9)], 0), preferred_element_type=F32) + bias2
                half = [jnp.dot(
                    jnp.concatenate([jnp.concatenate([lhs(cur, prv, n, m, j) for n in range(9, 15)], 1) for j in range(3)], 0),
                    jnp.concatenate([tile(l, n, m) for n in range(9, 15)], 0), preferred_element_type=F32) for m in range(2)]
                for e in range(2):
                    for r in range(7):
                        norm_row(src, nxt, q + 2, e, r, coef)
                for e in range(2):
                    for j in range(3):
                        sums = finish(q, e, j, full, half[e], sums)
            return sums

        for q in range(2):
            for e in range(2):
                for r in range(7):
                    norm_row(src, acts[q], q, e, r, coef)
        zero = jnp.zeros((8, C), F32)
        sums = lax.fori_loop(0, TRIPS, trip, (zero, zero))
        if last:
            out_copy(3).start()
        else:
            row_copy(l + 1, 3).start()
        for c in range(5):
            row_copy(l, c).wait_send()
        frame_copy(l).wait_send()
        if last:
            out_copy(4).start()
        return sums

    def body():
        blank = jnp.zeros((W, C), BF)
        for act in acts:
            for dj in range(3):
                for e in range(2):
                    for r in (0, 7):
                        act[dj, e, r] = blank

        sums = (jnp.zeros((8, C), F32), jnp.zeros((8, C), F32))
        for c, (f, n) in enumerate(CHUNKS):
            x_load(c).wait()

            def add(i, sums, f=f):
                s1, s2 = sums
                for r in range(ROWS):
                    v = buf_a[f + i, r].astype(F32)
                    s1 = s1 + sum8(v)
                    s2 = s2 + sum8(v * v)
                return s1, s2

            sums = lax.fori_loop(0, n, add, sums)

        pl.semaphore_wait(barrier, n_cp)
        for l in range(4):
            def mid(l=l):
                if l == 0:
                    for c in range(5):
                        row_copy(0, c).start()
                else:
                    row_copy(l, 4).start()

            part = reduce_stats(l, *sums, mid)
            w_load(l).wait()
            if l == 0:
                row_copy(0, 0).wait_recv()
                frame_copy(0).start()
            sums = layer(l, coefficients(l, part))
        for c in range(5):
            out_copy(c).wait()

    body()


def solution(mesh):
    n_cp, n_hp = mesh.shape["cp"], mesh.shape["hp"]

    def local(lat, conv_w, conv_b, gn_gamma, gn_beta):
        count = float(FRAMES * n_cp * ROWS * n_hp * W * (C // GROUPS))
        any_spec = pl.BlockSpec(memory_space=pl.ANY)
        vmem = pl.BlockSpec(memory_space=pltpu.VMEM)
        dma = pltpu.SemaphoreType.DMA
        return pl.pallas_call(
            functools.partial(kernel, count, n_cp),
            out_shape=jax.ShapeDtypeStruct((FRAMES, ROWS, W, C), BF),
            in_specs=[any_spec, any_spec, vmem, vmem, vmem],
            out_specs=any_spec,
            scratch_shapes=[
                pltpu.VMEM((FRAMES + 4, ROWS + 1, W, C), BF),
                pltpu.VMEM((FRAMES + 4, ROWS + 1, W, C), BF),
                pltpu.VMEM((3, 2, ROWS + 2, W, C), BF),
                pltpu.VMEM((3, 2, ROWS + 2, W, C), BF),
                pltpu.VMEM((3, 2, ROWS + 2, W, C), BF),
                pltpu.VMEM((4, 27, C, C), BF),
                pltpu.VMEM((2, 2, 2, C), F32),
                pltpu.VMEM((2, n_cp + 1, 2, C), F32),
                dma((5,)), dma((4,)), dma((5,)),
                dma((4, 5)), dma((4, 5)), dma((4,)), dma((4,)),
                dma((2, n_cp + 1)), dma((2, n_cp + 1)),
            ],
            compiler_params=pltpu.CompilerParams(collective_id=0, has_side_effects=True, vmem_limit_bytes=60 * 2**20),
        )(lat, conv_w.reshape(4, 27, C, C), conv_b, gn_gamma, gn_beta)

    video = P(("dp", "cp"), "hp", None, None)
    return jax.shard_map(local, mesh=mesh, in_specs=(video, P(), P(), P(), P()), out_specs=video, check_vma=False)
```

```python
import functools

import jax
import jax.numpy as jnp
from jax import lax
from jax.experimental import pallas as pl
from jax.experimental.pallas import tpu as pltpu
from jax.sharding import PartitionSpec as P

MESH = pl.DeviceIdType.MESH
GROUPS = 32
EPS = 1e-6
FRAMES = 24
ROWS = 6
W = 128
C = 128
TRIPS = 4
CHUNKS = ((22, 4), (16, 6), (10, 6), (4, 6), (2, 2))
SIDE = 64
BF = jnp.bfloat16
F32 = jnp.float32


def kernel(count, n_cp, lat, w_hbm, bias, gamma, beta, out, buf_a, buf_b, act0, act1, act2, wts, stat_out, stat_in,
           x_sem, w_sem, out_sem, row_send, row_recv, frame_send, frame_recv, stat_send, stat_recv):
    me = lax.axis_index("cp")
    hp = lax.axis_index("hp")
    acts = (act0, act1, act2)
    partner = {"hp": 1 - hp}
    after = {"cp": (me + 1) % n_cp}

    half = n_cp // 2

    def outward(step):
        lax.fori_loop(0, half, lambda j, n: step((me + half + j) % n_cp, n), 0)
        lax.fori_loop(1, half, lambda j, n: step((me + j) % n_cp, n), 0)

    def inward(step):
        lax.fori_loop(1, half, lambda j, n: step((me + j) % n_cp, n), 0)
        lax.fori_loop(0, half, lambda j, n: step((me + n_cp - 1 - j) % n_cp, n), 0)

    def x_load(c):
        f, n = CHUNKS[c]
        return pltpu.make_async_copy(lat.at[pl.ds(f - 2, n)], buf_a.at[pl.ds(f, n), pl.ds(0, ROWS)], x_sem.at[c])

    def w_load(l):
        return pltpu.make_async_copy(w_hbm.at[l], wts.at[l], w_sem.at[l])

    for c in range(5):
        x_load(c).start()
    for l in range(4):
        w_load(l).start()

    barrier = pltpu.get_barrier_semaphore()
    def greet(p, n):
        pl.semaphore_signal(barrier, inc=1, device_id={"cp": p}, device_id_type=MESH)
        return n

    pl.semaphore_signal(barrier, inc=1, device_id=partner, device_id_type=MESH)
    outward(greet)

    def row_copy(s, c):
        buf = (buf_a, buf_b)[s % 2]
        f, n = CHUNKS[c]
        edge = (ROWS - 1) * (1 - hp)
        return pltpu.make_async_remote_copy(
            src_ref=buf.at[pl.ds(f, n), pl.ds(edge, 1)], dst_ref=buf.at[pl.ds(f, n), pl.ds(ROWS, 1)],
            send_sem=row_send.at[s, c], recv_sem=row_recv.at[s, c], device_id=partner, device_id_type=MESH)

    def frame_copy(s):
        buf = (buf_a, buf_b)[s % 2]
        return pltpu.make_async_remote_copy(
            src_ref=buf.at[pl.ds(24, 2)], dst_ref=buf.at[pl.ds(0, 2)],
            send_sem=frame_send.at[s], recv_sem=frame_recv.at[s], device_id=after, device_id_type=MESH)

    def out_copy(c):
        f, n = CHUNKS[c]
        return pltpu.make_async_copy(buf_a.at[pl.ds(f, n), pl.ds(0, ROWS)], out.at[pl.ds(f - 2, n)], out_sem.at[c])

    def chip_copy(s, p, slot):
        return pltpu.make_async_remote_copy(
            src_ref=stat_out.at[s % 2, 0], dst_ref=stat_in.at[s % 2, slot], send_sem=stat_send.at[s % 2, p],
            recv_sem=stat_recv.at[s % 2, slot], device_id={"cp": p}, device_id_type=MESH)

    def core_copy(s):
        return pltpu.make_async_remote_copy(
            src_ref=stat_out.at[s % 2, 1], dst_ref=stat_in.at[s % 2, n_cp], send_sem=stat_send.at[s % 2, n_cp],
            recv_sem=stat_recv.at[s % 2, n_cp], device_id=partner, device_id_type=MESH)

    row_id = lax.broadcasted_iota(jnp.int32, (8, C), 0)
    lane_id = lax.broadcasted_iota(jnp.int32, (8, C), 1)

    def reduce_stats(s, s1, s2, mid):
        part = jnp.concatenate([jnp.sum(s1, axis=0, keepdims=True), jnp.sum(s2, axis=0, keepdims=True)], 0)
        stat_out[s % 2, 0] = part
        stat_in[s % 2, me] = part

        def send(p, n):
            chip_copy(s, p, me).start()
            return n

        def sent(p, n):
            chip_copy(s, p, p).wait_send()
            return n

        def landed(p, n):
            chip_copy(s, p, p).wait_recv()
            return n

        outward(send)
        mid()
        outward(sent)
        inward(landed)
        terms = [stat_in[s % 2, i] for i in range(n_cp)]
        while len(terms) > 1:
            terms = [a + b for a, b in zip(terms[::2], terms[1::2])]
        stat_out[s % 2, 1] = terms[0]
        core_copy(s).start()
        core_copy(s).wait()
        return terms[0] + stat_in[s % 2, n_cp]

    def coefficients(l, part):
        part = jnp.where(row_id == 0, part[0:1], part[1:2])
        pair = part + jnp.where(lane_id % 2 == 0, pltpu.roll(part, C - 1, 1), pltpu.roll(part, 1, 1))
        group = pair + jnp.where(lane_id % 4 < 2, pltpu.roll(pair, C - 2, 1), pltpu.roll(pair, 2, 1))
        mean = group[0:1] / count
        var = group[1:2] / count - mean * mean
        inv = lax.rsqrt(var + EPS)
        g = gamma[l:l + 1]
        scale = inv * g
        shift = beta[l:l + 1] - mean * inv * g
        return jnp.broadcast_to(0.5 * scale, (8, C)), jnp.broadcast_to(0.5 * shift, (8, C))

    col8 = lax.broadcasted_iota(jnp.int32, (W, C), 0)
    halo_row = 7 * (1 - hp)

    def norm_row(src, dst, q, e, r, coef):
        scale, shift = coef
        f = jnp.maximum(24 - 2 * q, 0) + e
        f = jnp.where((q >= 12) & (me == 0), 2, f)
        v = src[f, r].astype(F32).reshape(W // 8, 8, C)
        u = (v * scale[None] + shift[None]).reshape(W, C)
        a = u + u * jnp.tanh(u)
        row = halo_row if r == ROWS else r + 1
        dst[1, e, row] = a.astype(BF)
        dst[0, e, row] = jnp.where(col8 == 0, 0.0, pltpu.roll(a, 1, 0)).astype(BF)
        dst[2, e, row] = jnp.where(col8 == W - 1, 0.0, pltpu.roll(a, W - 1, 0)).astype(BF)

    def tile(l, n, m):
        def w(k, di, dj):
            return wts[l, k * 9 + di * 3 + dj]

        def block(a, b, c, d):
            return jnp.concatenate([jnp.concatenate([a, b], 1), jnp.concatenate([c, d], 1)], 0)

        if n < 9:
            di, dj = n // 3, n % 3
            return block(w(1, di, dj), w(0, di, dj), w(2, di, dj), w(1, di, dj))
        dj, half = (n - 9) % 3, (n - 9) // 3
        k = 0 if m == 0 else 2
        if half == 0:
            return block(w(k, 1, dj), w(k, 0, dj), w(k, 2, dj), w(k, 1, dj))
        zero = jnp.zeros((C, C), BF)
        return block(w(k, 0, dj), zero, zero, w(k, 2, dj))

    def lhs(cur, prv, n, m, j):
        if n < 9:
            di, dj = n // 3, n % 3
            i = 3 * m + j + di
            return jnp.concatenate([prv[dj, 1, i], cur[dj, 0, i]], 1)
        dj, half = (n - 9) % 3, (n - 9) // 3
        frame = prv.at[dj, 0] if m == 0 else cur.at[dj, 1]
        i = 2 * j
        if half == 0:
            return jnp.concatenate([frame[i + 1], frame[i + 2]], 1)
        return jnp.concatenate([frame[i], frame[i + 3]], 1)

    def sum8(v):
        return jnp.sum(v.reshape(W // 8, 8, C), axis=0)

    def layer(l, coef):
        src = (buf_a, buf_b)[l % 2]
        dst = (buf_a, buf_b)[1 - l % 2]
        residual = l % 2 == 1
        last = l == 3
        bias2 = jnp.concatenate([bias[l:l + 1], bias[l:l + 1]], 1)

        def finish(q, e, j, full, v, sums):
            f = 24 - 2 * q + e
            s1, s2 = sums
            for half in range(2):
                o = 2 * j + half
                h = (full[o * W:(o + 1) * W, e * C:(e + 1) * C] + v[j * W:(j + 1) * W, half * C:(half + 1) * C]).astype(BF)
                if residual:
                    h = (dst[f, o].astype(F32) + h.astype(F32)).astype(BF)
                dst[f, o] = h
                if not last:
                    hf = h.astype(F32)
                    s1 = s1 + sum8(hf)
                    s2 = s2 + sum8(hf * hf)
            return s1, s2

        def trip(it, sums):
            def wait_rows(c):
                row_copy(l, c).wait_recv()

            for i in range(3):
                @pl.when(it == i)
                def _(i=i):
                    wait_rows(i + 1)

            @pl.when(it == 3)
            def _():
                wait_rows(4)
                frame_copy(l).wait_recv()

            for i in range(1, 4):
                @pl.when(it == i)
                def _(i=i):
                    if last:
                        out_copy(i - 1).start()
                    else:
                        row_copy(l + 1, i - 1).start()
                        if i == 2:
                            row_copy(l + 1, 0).wait_recv()
                            frame_copy(l + 1).start()

            for k in range(3):
                q = 3 * it + k
                cur, prv, nxt = acts[k], acts[(k + 1) % 3], acts[(k + 2) % 3]
                full = jnp.dot(
                    jnp.concatenate([jnp.concatenate([lhs(cur, prv, n, m, j) for n in range(9)], 1) for m in range(2) for j in range(3)], 0),
                    jnp.concatenate([tile(l, n, 0) for n in range(9)], 0), preferred_element_type=F32) + bias2
                half = [jnp.dot(
                    jnp.concatenate([jnp.concatenate([lhs(cur, prv, n, m, j) for n in range(9, 15)], 1) for j in range(3)], 0),
                    jnp.concatenate([tile(l, n, m) for n in range(9, 15)], 0), preferred_element_type=F32) for m in range(2)]
                for e in range(2):
                    for r in range(7):
                        norm_row(src, nxt, q + 2, e, r, coef)
                for e in range(2):
                    for j in range(3):
                        sums = finish(q, e, j, full, half[e], sums)
            return sums

        for q in range(2):
            for e in range(2):
                for r in range(7):
                    norm_row(src, acts[q], q, e, r, coef)
        zero = jnp.zeros((8, C), F32)
        sums = lax.fori_loop(0, TRIPS, trip, (zero, zero))
        if last:
            out_copy(3).start()
        else:
            row_copy(l + 1, 3).start()
        for c in range(5):
            row_copy(l, c).wait_send()
        frame_copy(l).wait_send()
        if last:
            out_copy(4).start()
        return sums

    def body():
        blank = jnp.zeros((W, C), BF)
        for act in acts:
            for dj in range(3):
                for e in range(2):
                    for r in (0, 7):
                        act[dj, e, r] = blank

        sums = (jnp.zeros((8, C), F32), jnp.zeros((8, C), F32))
        for c, (f, n) in enumerate(CHUNKS):
            x_load(c).wait()

            def add(i, sums, f=f):
                s1, s2 = sums
                for r in range(ROWS):
                    v = buf_a[f + i, r].astype(F32)
                    s1 = s1 + sum8(v)
                    s2 = s2 + sum8(v * v)
                return s1, s2

            sums = lax.fori_loop(0, n, add, sums)

        pl.semaphore_wait(barrier, n_cp)
        for l in range(4):
            def mid(l=l):
                if l == 0:
                    for c in range(5):
                        row_copy(0, c).start()
                else:
                    row_copy(l, 4).start()

            part = reduce_stats(l, *sums, mid)
            w_load(l).wait()
            if l == 0:
                row_copy(0, 0).wait_recv()
                frame_copy(0).start()
            sums = layer(l, coefficients(l, part))
        for c in range(5):
            out_copy(c).wait()

    body()


def hand_over(src, dst):
    dst[...] = src[...]


def solution(mesh):
    n_cp, n_hp = mesh.shape["cp"], mesh.shape["hp"]

    def local(lat, conv_w, conv_b, gn_gamma, gn_beta):
        count = float(FRAMES * n_cp * ROWS * n_hp * W * (C // GROUPS))
        any_spec = pl.BlockSpec(memory_space=pl.ANY)
        vmem = pl.BlockSpec(memory_space=pltpu.VMEM)
        dma = pltpu.SemaphoreType.DMA
        decoded = pl.pallas_call(
            functools.partial(kernel, count, n_cp),
            out_shape=jax.ShapeDtypeStruct((FRAMES, ROWS, W, C), BF),
            in_specs=[any_spec, any_spec, vmem, vmem, vmem],
            out_specs=any_spec,
            scratch_shapes=[
                pltpu.VMEM((FRAMES + 4, ROWS + 1, W, C), BF),
                pltpu.VMEM((FRAMES + 4, ROWS + 1, W, C), BF),
                pltpu.VMEM((3, 2, ROWS + 2, W, C), BF),
                pltpu.VMEM((3, 2, ROWS + 2, W, C), BF),
                pltpu.VMEM((3, 2, ROWS + 2, W, C), BF),
                pltpu.VMEM((4, 27, C, C), BF),
                pltpu.VMEM((2, 2, 2, C), F32),
                pltpu.VMEM((2, n_cp + 1, 2, C), F32),
                dma((5,)), dma((4,)), dma((5,)),
                dma((4, 5)), dma((4, 5)), dma((4,)), dma((4,)),
                dma((2, n_cp + 1)), dma((2, n_cp + 1)),
            ],
            compiler_params=pltpu.CompilerParams(collective_id=0, has_side_effects=True, vmem_limit_bytes=60 * 2**20),
        )(lat, conv_w.reshape(4, 27, C, C), conv_b, gn_gamma, gn_beta)
        block = pl.BlockSpec((3, ROWS, W, C), lambda i: (i, 0, 0, 0))
        return pl.pallas_call(
            hand_over, grid=(FRAMES // 3,), out_shape=jax.ShapeDtypeStruct((FRAMES, ROWS, W, C), BF),
            in_specs=[block], out_specs=block)(decoded)

    video = P(("dp", "cp"), "hp", None, None)
    return jax.shard_map(local, mesh=mesh, in_specs=(video, P(), P(), P(), P()), out_specs=video, check_vma=False)
```
